128 devices in a mesh: gx: 16 (over z, x), gy: 4 (over y_hi, core), gz: 2 (over y_lo).
Axes of the slice: x: 4, y: 4 (y_hi: 2, y_lo: 2; y = y_hi * 2 + y_lo), z: 4, core: 2. Of those that a mesh axis runs over, the one named last changes fastest.
Arguments:
- hidden: bfloat16 [49152, 4608], P(('gx', 'gy', 'gz')), may hold values from -24 to 24
- out_grad: bfloat16 [49152, 1152], P(('gx', 'gy', 'gz')), may hold values from -6 to 6
- down_weight: bfloat16 [4608, 1152], replicated, may hold values from -0.1875 to 0.1875
Outputs:
- weight_grad: float32 [4608, 1152], P(('gx', 'gy', 'gz'))
- hidden_grad: bfloat16 [49152, 4608], P(('gx', 'gy', 'gz'))
The draws below stay inside these ranges and needn't reach their ends.
All inputs are finite; a program needn't handle non-finite values.
Results may differ from the reference program's by a relative error of at most 0.001.
Values may be sent and summed in bfloat16 or wider, within the bound.
No kernel may reach another device: no remote copies, remote signals or barrier semaphores. Data moves between devices by JAX's collectives and lax.ppermute only.
A program may use at most 128 MiB of HBM per device.

```python
import jax
import jax.numpy as jnp
from jax import lax

FFW = 4608
DW = 1152
TOKENS = 49152


def strengthened(array, rng, source, target, shards_of, factor):
    owner, partner = [(jnp.arange(array.shape[dim]) // (array.shape[dim] // shards_of)).reshape([-1 if axis == dim else 1 for axis in range(array.ndim)]) for dim in (source, target)]
    chosen = jax.random.permutation(rng, shards_of)[partner]
    strong = (owner == chosen) | (owner == (partner + shards_of // 2) % shards_of)
    return jnp.where(strong, factor * array, array)


def block_scale(rng, dims, split, least, largest):
    level = 1.0
    for axis_at, shards_of in split:
        draws = jax.random.uniform(jax.random.fold_in(jax.random.fold_in(rng, 6), axis_at), (shards_of,), jnp.float32, least / len(split), largest / len(split))
        level = level * jnp.repeat(jnp.exp(draws), dims[axis_at] // shards_of).reshape((-1,) + (1,) * (len(dims) - 1 - axis_at))
    return level


def centred(own_key, dims, width, most, cuts=(), kind=jnp.bfloat16):
    drawn = jax.random.normal(own_key, dims, jnp.float32) * width
    if len(cuts) > 0:
        drawn = block_scale(own_key, dims, cuts, -0.22, 0.18) * drawn
    return jnp.clip(drawn, min=-most, max=most).astype(kind)


def heavy_noise(rng, shape, deviation, reach, cuts, heavy, kind=jnp.bfloat16):
    values = deviation * jax.random.normal(rng, shape, jnp.float32)
    if cuts:
        values = values * block_scale(rng, shape, cuts, -0.22, 0.18)
    return jnp.clip(strengthened(values, jax.random.fold_in(rng, 3), *heavy), -reach, reach).astype(kind)


def setup_inputs(seed: int = 0) -> dict:
    splits = jax.random.split(jax.random.key(seed), 4)
    hidden = heavy_noise(splits[0], (TOKENS, FFW), 1.0, 24.0, ((0, 128),), (0, 1, 128, 5.5))
    out_grad = centred(splits[1], (TOKENS, DW), 1.0, 6.0, ((0, 128),))
    down_weight = centred(splits[2], (FFW, DW), DW ** -0.5, 0.1875)
    return {"hidden": hidden, "out_grad": out_grad, "down_weight": down_weight}


def reference(hidden, out_grad, down_weight):
    summed = lax.dot_general(hidden, out_grad, (((0,), (0,)), ((), ())), preferred_element_type=jnp.float32)
    weight_grad = summed / jnp.sqrt(jnp.float32(TOKENS))
    hidden_grad = lax.dot_general(out_grad, down_weight, (((1,), (1,)), ((), ())), preferred_element_type=jnp.float32)
    return (weight_grad, hidden_grad.astype(jnp.bfloat16))
```

```python
import functools

import jax
import jax.numpy as jnp
from jax import lax
from jax.experimental import pallas as pl
from jax.experimental.pallas import tpu as pltpu
from jax.sharding import PartitionSpec as P

AXES = ("gx", "gy", "gz")
SIDE = 4
BLOCK = 36
PADDED = 40
TAIL = 8
WIDE = 768
NARROW = 384


def position(index):
    return index >> 5, index >> 3 & 3, index >> 1 & 2 | index & 1, index >> 1 & 1


def device(z, x, y, core):
    return ((z * 4 + x) * 4 + y // 2 * 2 + core) * 2 + y % 2


def routes(dims, step):
    pairs = []
    for source in range(128):
        at = dict(zip("zxyc", position(source)))
        along = dims[at["c"]]
        at[along] = (at[along] + step) % SIDE
        pairs.append((source, device(at["z"], at["x"], at["y"], at["c"])))
    return pairs


def across_cores(array):
    pairs = []
    for source in range(128):
        z, x, y, core = position(source)
        pairs.append((source, device(z, x, y, 1 - core)))
    return lax.ppermute(array, AXES, pairs)


def turn_body(where, hidden, send, keep):
    core = position(where[0])[3]
    turned = hidden[...].T
    for x in range(SIDE):
        rows = 288 * x
        piece = jnp.concatenate([turned[rows : rows + 72], turned[rows + 144 : rows + 216]], 0)

        @pl.when(core == 0)
        def _():
            keep[x] = piece

        @pl.when(core == 1)
        def _():
            send[x] = piece

    for y in range(SIDE):
        rows = 144 * (y // 2) + 72 + BLOCK * (y % 2)
        piece = jnp.concatenate(
            [turned[288 * x + rows : 288 * x + rows + BLOCK] for x in range(SIDE)], 0
        )

        @pl.when(core == 1)
        def _():
            keep[y] = piece

        @pl.when(core == 0)
        def _():
            send[y] = piece


def turn(where, hidden):
    tokens, width = hidden.shape
    out = jax.ShapeDtypeStruct((SIDE, width // 8, tokens), hidden.dtype)
    return pl.pallas_call(
        turn_body,
        grid=(SIDE,),
        in_specs=[
            pl.BlockSpec(memory_space=pltpu.SMEM),
            pl.BlockSpec((tokens, width // SIDE), lambda b: (0, b)),
        ],
        out_specs=[pl.BlockSpec((SIDE, width // 32, tokens), lambda b: (0, b, 0))] * 2,
        out_shape=[out, out],
        cost_estimate=pl.CostEstimate(flops=2 * 10**9, bytes_accessed=7 * 10**6, transcendentals=0),
    )(where, hidden)


def largest(values):
    return jnp.max(jnp.max(values, axis=0, keepdims=True).astype(jnp.float32))


def product_body(step, where, mine, other, grad, other_grad, *refs):
    if step == 1:
        wide, narrow, level = refs
        top = largest(jnp.maximum(jnp.abs(mine[...]), jnp.abs(other[...])).reshape(-1, mine.shape[2]))
        grad_top = largest(jnp.maximum(jnp.abs(grad[...]), jnp.abs(other_grad[...])))
        tokens = grad.shape[0] * 2
        bound = jnp.full((TAIL, 128), 1.0, jnp.float32)
        bound = bound * (top * grad_top * tokens)
        bits = 15.0 - jnp.ceil(jnp.log2(jnp.maximum(bound, 2.0**-60)))
        level[...] = bits
    else:
        given, wide, narrow = refs
        bits = given[...]
    scale = jnp.exp2(bits)[0:1, 0:1]
    z, x, y, core = position(where[0])
    at = jnp.where(core == 0, x, y) + step & 3
    left = jnp.concatenate([mine[at], other[at]], 1)
    both = jnp.concatenate([grad[...], other_grad[...]], 0)
    row = pl.multiple_of((z + step & 3) * 144, 16)
    cut = jnp.concatenate(
        [
            jnp.concatenate([source[t, pl.ds(row, 144)] for t in range(SIDE)], 0)
            for source in (mine, other)
        ],
        1,
    )
    one = jnp.dot(left, both[:, :WIDE], preferred_element_type=jnp.float32)
    two = jnp.dot(cut, both[:, WIDE:], preferred_element_type=jnp.float32)
    wide[0:576] = one * scale
    narrow[0:576] = two * scale
    wide[576:] = jnp.broadcast_to(bits[:, 0:1], (TAIL, WIDE))
    narrow[576:] = jnp.broadcast_to(bits[:, 0:1], (TAIL, NARROW))


def product(step, where, mine, other, grad, other_grad, level=None):
    first = step == 1
    outs = [
        jax.ShapeDtypeStruct((576 + TAIL, WIDE), jnp.float32),
        jax.ShapeDtypeStruct((576 + TAIL, NARROW), jnp.float32),
    ]
    if first:
        outs.append(jax.ShapeDtypeStruct((TAIL, 128), jnp.float32))
    n = 4 if first else 5
    return pl.pallas_call(
        functools.partial(product_body, step),
        in_specs=[pl.BlockSpec(memory_space=pltpu.SMEM)] + [pl.BlockSpec(memory_space=pltpu.VMEM)] * n,
        out_specs=[pl.BlockSpec(memory_space=pltpu.VMEM)] * len(outs),
        out_shape=outs,
        cost_estimate=pl.CostEstimate(flops=10**9, bytes_accessed=5 * 10**6, transcendentals=0),
    )(where, mine, other, grad, other_grad, *([] if first else [level]))


def gather_sum(parts, rows):
    total, least = None, None
    for part in parts:
        bits = part[rows : rows + TAIL, 0:128]
        value = part[0:rows] * jnp.exp2(-bits)[0:1, 0:1]
        total = value if total is None else total + value
        least = bits if least is None else jnp.minimum(least, bits)
    return total, least - 2.0


def spread_body(rows, blocks, stride, where, *refs):
    z, x, y, core = position(where[0])
    if blocks == 16:
        ways = (
            (jnp.where(core == 0, z, x), jnp.where(core == 0, 4, 1), jnp.where(core == 0, 1, 4)),
            (y, jnp.where(core == 0, 1, 4), jnp.where(core == 0, 4, 1)),
        )
    else:
        ways = ((jnp.where(core == 0, y, z), 1, 0), (x, 1, 0))
    for p, width in enumerate((WIDE, NARROW)):
        parts, out, scratch = refs[4 * p : 4 * p + 4], refs[8 + p], refs[10 + p]
        total, bits = gather_sum(parts, rows)
        scale = jnp.exp2(bits)[0:1, 0:1]
        for i in range(blocks):
            scratch[i, 0:BLOCK] = total[stride * i : stride * i + BLOCK]
            scratch[i, BLOCK:] = jnp.zeros((PADDED - BLOCK, width), jnp.float32)
        at, major, minor = ways[p]
        for k in range(SIDE):
            chunk = at + k & 3
            for t in range(blocks // SIDE):
                out[k, PADDED * t : PADDED * (t + 1)] = scratch[chunk * major + t * minor] * scale
            out[k, PADDED * blocks // SIDE :] = jnp.broadcast_to(bits[:, 0:1], (TAIL, width))


def spread(where, rows, blocks, stride, wide, narrow):
    high = PADDED * blocks // SIDE + TAIL
    return pl.pallas_call(
        functools.partial(spread_body, rows, blocks, stride),
        in_specs=[pl.BlockSpec(memory_space=pltpu.SMEM)] + [pl.BlockSpec(memory_space=pltpu.VMEM)] * 8,
        out_specs=[pl.BlockSpec(memory_space=pltpu.VMEM)] * 2,
        out_shape=[
            jax.ShapeDtypeStruct((SIDE, high, WIDE), jnp.float32),
            jax.ShapeDtypeStruct((SIDE, high, NARROW), jnp.float32),
        ],
        scratch_shapes=[
            pltpu.VMEM((blocks, PADDED, WIDE), jnp.float32),
            pltpu.VMEM((blocks, PADDED, NARROW), jnp.float32),
        ],
        cost_estimate=pl.CostEstimate(flops=10**8, bytes_accessed=10**7, transcendentals=0),
    )(where, *wide, *narrow)


def finish_body(factor, *refs):
    out = refs[8]
    for p, (low, high) in enumerate(((0, WIDE), (WIDE, WIDE + NARROW))):
        total, _ = gather_sum(refs[4 * p : 4 * p + 4], PADDED)
        out[:, low:high] = total[0:BLOCK] * factor


def finish(factor, wide, narrow):
    return pl.pallas_call(
        functools.partial(finish_body, factor),
        in_specs=[pl.BlockSpec(memory_space=pltpu.VMEM)] * 8,
        out_specs=pl.BlockSpec(memory_space=pltpu.VMEM),
        out_shape=jax.ShapeDtypeStruct((BLOCK, WIDE + NARROW), jnp.float32),
    )(*wide, *narrow)


def exchange(chunks, dims):
    return {k: lax.ppermute(chunks[k].astype(jnp.float16), AXES, routes(dims, k)) for k in chunks}


def body(hidden, out_grad, down_weight):
    where = lax.axis_index(AXES).reshape(1)
    tokens = hidden.shape[0] * 128
    factor = 1.0 / float(tokens) ** 0.5

    other_grad = across_cores(out_grad)
    send, keep = turn(where, hidden)
    got = across_cores(send)

    level = None
    wide, narrow = {}, {}
    from_wide, from_narrow = {}, {}
    for k in (1, 3, 2, 0):
        outs = product(k, where, keep, got, out_grad, other_grad, level)
        if level is None:
            level = outs[2]
        wide[k], narrow[k] = outs[0], outs[1]
        if k:
            from_wide |= exchange({k: wide[k]}, "xy")
            from_narrow |= exchange({k: narrow[k]}, "zz")

    hidden_grad = lax.dot_general(
        out_grad, down_weight, (((1,), (1,)), ((), ())), preferred_element_type=jnp.float32
    ).astype(jnp.bfloat16)

    wide, narrow = spread(
        where, 576, 16, BLOCK,
        [wide[0]] + [from_wide[k].astype(jnp.float32) for k in (1, 2, 3)],
        [narrow[0]] + [from_narrow[k].astype(jnp.float32) for k in (1, 2, 3)],
    )
    from_wide = exchange({k: wide[k] for k in (1, 3, 2)}, "zx")
    from_narrow = exchange({k: narrow[k] for k in (1, 3, 2)}, "yy")

    wide, narrow = spread(
        where, 160, 4, PADDED,
        [wide[0]] + [from_wide[k].astype(jnp.float32) for k in (1, 2, 3)],
        [narrow[0]] + [from_narrow[k].astype(jnp.float32) for k in (1, 2, 3)],
    )
    from_wide = exchange({k: wide[k] for k in (1, 3, 2)}, "yz")
    from_narrow = exchange({k: narrow[k] for k in (1, 3, 2)}, "xx")

    weight_grad = finish(
        factor,
        [wide[0]] + [from_wide[k].astype(jnp.float32) for k in (1, 2, 3)],
        [narrow[0]] + [from_narrow[k].astype(jnp.float32) for k in (1, 2, 3)],
    )
    return (weight_grad, hidden_grad)


def solution(mesh):
    in_specs = (P(AXES, None), P(AXES, None), P())
    out_specs = (P(AXES, None), P(AXES, None))
    return jax.shard_map(body, mesh=mesh, in_specs=in_specs, out_specs=out_specs, check_vma=False)
```

```python
import functools

import jax
import jax.numpy as jnp
from jax import lax
from jax.experimental import pallas as pl
from jax.experimental.pallas import tpu as pltpu
from jax.sharding import PartitionSpec as P


AXES = ("gx", "gy", "gz")
SIDE = 4
BLOCK = 36
PADDED = 40
TAIL = 8
WIDE = 768
NARROW = 384


def near(array):
    return pltpu.with_memory_space_constraint(array, pltpu.VMEM)


def position(index):
    return index >> 5, index >> 3 & 3, index >> 1 & 2 | index & 1, index >> 1 & 1


def device(z, x, y, core):
    return ((z * 4 + x) * 4 + y // 2 * 2 + core) * 2 + y % 2


def routes(dims, step):
    pairs = []
    for source in range(128):
        at = dict(zip("zxyc", position(source)))
        along = dims[at["c"]]
        at[along] = (at[along] + step) % SIDE
        pairs.append((source, device(at["z"], at["x"], at["y"], at["c"])))
    return pairs


def across_cores(array):
    pairs = []
    for source in range(128):
        z, x, y, core = position(source)
        pairs.append((source, device(z, x, y, 1 - core)))
    return lax.ppermute(array, AXES, pairs)


def turn_body(where, hidden, send, keep):
    core = position(where[0])[3]
    turned = hidden[...].T
    for x in range(SIDE):
        rows = 288 * x
        piece = jnp.concatenate([turned[rows : rows + 72], turned[rows + 144 : rows + 216]], 0)

        @pl.when(core == 0)
        def _():
            keep[x] = piece

        @pl.when(core == 1)
        def _():
            send[x] = piece

    for y in range(SIDE):
        rows = 144 * (y // 2) + 72 + BLOCK * (y % 2)
        piece = jnp.concatenate(
            [turned[288 * x + rows : 288 * x + rows + BLOCK] for x in range(SIDE)], 0
        )

        @pl.when(core == 1)
        def _():
            keep[y] = piece

        @pl.when(core == 0)
        def _():
            send[y] = piece


def turn(where, hidden):
    tokens, width = hidden.shape
    out = pltpu.VMEM((SIDE, width // 8, tokens), hidden.dtype)
    return pl.pallas_call(
        turn_body,
        grid=(SIDE,),
        in_specs=[
            pl.BlockSpec(memory_space=pltpu.SMEM),
            pl.BlockSpec((tokens, width // SIDE), lambda b: (0, b)),
        ],
        out_specs=[pl.BlockSpec((SIDE, width // 32, tokens), lambda b: (0, b, 0))] * 2,
        out_shape=[out, out],
        compiler_params=pltpu.CompilerParams(vmem_limit_bytes=16 * 2**20),
        cost_estimate=pl.CostEstimate(flops=2 * 10**9, bytes_accessed=7 * 10**6, transcendentals=0),
    )(where, pltpu.with_memory_space_constraint(hidden, pltpu.HBM))


def largest(values):
    return jnp.max(jnp.max(values, axis=0, keepdims=True).astype(jnp.float32))


def product_body(step, where, mine, other, grad, other_grad, *refs):
    if step == 1:
        wide, narrow, level = refs
        top = largest(jnp.maximum(jnp.abs(mine[...]), jnp.abs(other[...])).reshape(-1, mine.shape[2]))
        grad_top = largest(jnp.maximum(jnp.abs(grad[...]), jnp.abs(other_grad[...])))
        tokens = grad.shape[0] * 2
        bound = jnp.full((TAIL, 128), 1.0, jnp.float32)
        bound = bound * (top * grad_top * tokens)
        bits = 15.0 - jnp.ceil(jnp.log2(jnp.maximum(bound, 2.0**-60)))
        level[...] = bits
    else:
        given, wide, narrow = refs
        bits = given[...]
    scale = jnp.exp2(bits)[0:1, 0:1]
    z, x, y, core = position(where[0])
    at = jnp.where(core == 0, x, y) + step & 3
    left = jnp.concatenate([mine[at], other[at]], 1)
    both = jnp.concatenate([grad[...], other_grad[...]], 0)
    row = pl.multiple_of((z + step & 3) * 144, 16)
    cut = jnp.concatenate(
        [
            jnp.concatenate([source[t, pl.ds(row, 144)] for t in range(SIDE)], 0)
            for source in (mine, other)
        ],
        1,
    )
    one = jnp.dot(left, both[:, :WIDE], preferred_element_type=jnp.float32)
    two = jnp.dot(cut, both[:, WIDE:], preferred_element_type=jnp.float32)
    wide[0:576] = one * scale if step else one
    narrow[0:576] = two * scale if step else two
    wide[576:] = jnp.broadcast_to(bits[:, 0:1], (TAIL, WIDE))
    narrow[576:] = jnp.broadcast_to(bits[:, 0:1], (TAIL, NARROW))


def product(step, where, mine, other, grad, other_grad, level=None):
    first = step == 1
    outs = [
        pltpu.VMEM((576 + TAIL, WIDE), jnp.float32),
        pltpu.VMEM((576 + TAIL, NARROW), jnp.float32),
    ]
    if first:
        outs.append(pltpu.VMEM((TAIL, 128), jnp.float32))
    n = 4 if first else 5
    return pl.pallas_call(
        functools.partial(product_body, step),
        in_specs=[pl.BlockSpec(memory_space=pltpu.SMEM)] + [pl.BlockSpec(memory_space=pltpu.VMEM)] * n,
        out_specs=[pl.BlockSpec(memory_space=pltpu.VMEM)] * len(outs),
        out_shape=outs,
        compiler_params=pltpu.CompilerParams(vmem_limit_bytes=16 * 2**20),
        cost_estimate=pl.CostEstimate(flops=10**9, bytes_accessed=5 * 10**6, transcendentals=0),
    )(where, *map(near, [mine, other, grad, other_grad] + ([] if first else [level])))


def power(part, rows):
    return jnp.exp2(-part[rows : rows + 1].astype(jnp.float32))


def total(own, parts, rows):
    value = own[0:rows]
    for part in parts:
        value = value + part[0:rows].astype(jnp.float32) * power(part, rows)
    return value


def spread_body(blocks, stride, where, *refs):
    z, x, y, core = position(where[0])
    if blocks == 16:
        ways = (
            (jnp.where(core == 0, z, x), jnp.where(core == 0, 4, 1), jnp.where(core == 0, 1, 4)),
            (y, jnp.where(core == 0, 1, 4), jnp.where(core == 0, 4, 1)),
        )
    else:
        ways = ((jnp.where(core == 0, y, z), 1, 0), (x, 1, 0))
    for p, width in enumerate((WIDE, NARROW)):
        value, tails, out, scratch = refs[p], refs[2 + p], refs[4 + p], refs[6 + p]
        bits = jnp.min(tails[...], axis=0, keepdims=True) - 2.0
        scale = jnp.exp2(bits)[0:1, 0:1]
        for i in range(blocks):
            scratch[i, 0:BLOCK] = value[stride * i : stride * i + BLOCK]
            scratch[i, BLOCK:] = jnp.zeros((PADDED - BLOCK, width), jnp.float32)
        at, major, minor = ways[p]
        for k in range(SIDE):
            chunk = at + k & 3
            for t in range(blocks // SIDE):
                piece = scratch[chunk * major + t * minor]
                out[k, PADDED * t : PADDED * (t + 1)] = piece * scale if k else piece
            out[k, PADDED * blocks // SIDE :] = jnp.broadcast_to(bits[:, 0:1], (TAIL, width))


def spread(where, blocks, stride, wide, narrow, own_bits):
    high = PADDED * blocks // SIDE + TAIL
    rows = stride * blocks
    inputs = [total(*pair, rows) for pair in (wide, narrow)]
    for p, (_, parts) in enumerate((wide, narrow)):
        tails = [part[rows:, 0:128].astype(jnp.float32) for part in parts]
        inputs.append(jnp.concatenate([own_bits[p], *tails], 0))
    return pl.pallas_call(
        functools.partial(spread_body, blocks, stride),
        in_specs=[pl.BlockSpec(memory_space=pltpu.SMEM)] + [pl.BlockSpec(memory_space=pltpu.VMEM)] * 4,
        out_specs=[pl.BlockSpec(memory_space=pltpu.VMEM)] * 2,
        out_shape=[
            pltpu.VMEM((SIDE, high, WIDE), jnp.float32),
            pltpu.VMEM((SIDE, high, NARROW), jnp.float32),
        ],
        scratch_shapes=[
            pltpu.VMEM((blocks, PADDED, WIDE), jnp.float32),
            pltpu.VMEM((blocks, PADDED, NARROW), jnp.float32),
        ],
        compiler_params=pltpu.CompilerParams(vmem_limit_bytes=12 * 2**20),
        cost_estimate=pl.CostEstimate(flops=10**8, bytes_accessed=10**7, transcendentals=0),
    )(where, *map(near, inputs))


def exchange(chunks, dims):
    arrived = {}
    for k in chunks:
        arrived[k] = lax.ppermute(chunks[k].astype(jnp.float16), AXES, routes(dims, k))
    return arrived


def input_gradient_body(grad, weight, out):
    out[...] = lax.dot_general(
        grad[...], weight[...], (((1,), (1,)), ((), ())), preferred_element_type=jnp.float32
    ).astype(out.dtype)


def input_gradient(grad, weight):
    tokens, width = grad.shape
    features = weight.shape[0]
    step = 512
    return pl.pallas_call(
        input_gradient_body,
        grid=(features // step,),
        in_specs=[
            pl.BlockSpec((tokens, width), lambda i: (0, 0)),
            pl.BlockSpec((step, width), lambda i: (i, 0)),
        ],
        out_specs=pl.BlockSpec((tokens, step), lambda i: (0, i)),
        out_shape=pltpu.HBM((tokens, features), grad.dtype),
        compiler_params=pltpu.CompilerParams(vmem_limit_bytes=16 * 2**20),
        cost_estimate=pl.CostEstimate(
            flops=2 * tokens * width * features, bytes_accessed=15 * 10**6, transcendentals=0
        ),
    )(grad, pltpu.with_memory_space_constraint(weight, pltpu.HBM))


def listed(parts):
    return [parts[k] for k in (1, 2, 3)]


def body(hidden, out_grad, down_weight):
    where = lax.axis_index(AXES).reshape(1)
    tokens = hidden.shape[0] * 128
    factor = 1.0 / float(tokens) ** 0.5

    other_grad = across_cores(out_grad)
    send, keep = turn(where, hidden)
    got = across_cores(send)

    level = None
    wide, narrow = {}, {}
    from_wide, from_narrow = {}, {}
    for k in (1, 3, 2, 0):
        outs = product(k, where, keep, got, out_grad, other_grad, level)
        if level is None:
            level = outs[2]
        wide[k], narrow[k] = outs[0], outs[1]
        if k:
            from_wide |= exchange({k: wide[k]}, "xy")
            from_narrow |= exchange({k: narrow[k]}, "zz")

    hidden_grad = input_gradient(out_grad, down_weight)

    wide, narrow = spread(
        where, 16, BLOCK, (wide[0], listed(from_wide)), (narrow[0], listed(from_narrow)), (level, level)
    )
    from_wide = exchange({k: wide[k] for k in (1, 3, 2)}, "zx")
    from_narrow = exchange({k: narrow[k] for k in (1, 3, 2)}, "yy")

    own_bits = (wide[0, 160:, 0:128], narrow[0, 160:, 0:128])
    wide, narrow = spread(
        where, 4, PADDED, (wide[0], listed(from_wide)), (narrow[0], listed(from_narrow)), own_bits
    )
    from_wide = exchange({k: wide[k] for k in (1, 3, 2)}, "yz")
    from_narrow = exchange({k: narrow[k] for k in (1, 3, 2)}, "xx")

    sums = [
        total(own[0], listed(parts), PADDED)[0:BLOCK]
        for own, parts in ((wide, from_wide), (narrow, from_narrow))
    ]
    weight_grad = jnp.concatenate(sums, 1) * factor
    return (weight_grad, hidden_grad)


def solution(mesh):
    in_specs = (P(AXES, None), P(AXES, None), P())
    out_specs = (P(AXES, None), P(AXES, None))
    return jax.shard_map(body, mesh=mesh, in_specs=in_specs, out_specs=out_specs, check_vma=False)
```

```python
import functools

import jax
import jax.numpy as jnp
from jax import lax
from jax.experimental import pallas as pl
from jax.experimental.pallas import tpu as pltpu
from jax.sharding import PartitionSpec as P


AXES = ("gx", "gy", "gz")
SIDE = 4
BLOCK = 36
PADDED = 40
TAIL = 8
LATE = (2, 1, 3)
FIRST = {"wide": "xy", "narrow": "zz"}
SECOND = {"wide": "zx", "narrow": "yy"}
THIRD = {"wide": "yz", "narrow": "xx"}
PARTS = ("wide", "narrow")
WIDE = 768
NARROW = 384


def near(array):
    return pltpu.with_memory_space_constraint(array, pltpu.VMEM)


def position(index):
    return index >> 5, index >> 3 & 3, index >> 1 & 2 | index & 1, index >> 1 & 1


def device(z, x, y, core):
    return ((z * 4 + x) * 4 + y // 2 * 2 + core) * 2 + y % 2


def routes(dims, step):
    pairs = []
    for source in range(128):
        at = dict(zip("zxyc", position(source)))
        along = dims[at["c"]]
        at[along] = (at[along] + step) % SIDE
        pairs.append((source, device(at["z"], at["x"], at["y"], at["c"])))
    return pairs


def across_cores(array):
    pairs = []
    for source in range(128):
        z, x, y, core = position(source)
        pairs.append((source, device(z, x, y, 1 - core)))
    return lax.ppermute(array, AXES, pairs)


def turned_rows(block, b, core, send, keep):
    turned = block.T
    for x in range(SIDE):
        rows = 288 * x
        piece = jnp.concatenate([turned[rows : rows + 72], turned[rows + 144 : rows + 216]], 0)

        @pl.when(core == 0)
        def _():
            keep[x, 144 * b : 144 * (b + 1)] = piece

        @pl.when(core == 1)
        def _():
            send[x, 144 * b : 144 * (b + 1)] = piece

    for y in range(SIDE):
        rows = 144 * (y // 2) + 72 + BLOCK * (y % 2)
        piece = jnp.concatenate(
            [turned[288 * x + rows : 288 * x + rows + BLOCK] for x in range(SIDE)], 0
        )

        @pl.when(core == 1)
        def _():
            keep[y, 144 * b : 144 * (b + 1)] = piece

        @pl.when(core == 0)
        def _():
            send[y, 144 * b : 144 * (b + 1)] = piece


def highest(block, top):
    most = jnp.max(jnp.abs(block), axis=0, keepdims=True)
    return most if top is None else jnp.maximum(top, most)


def turn_first_body(tokens, where, hidden, send, keep, rest, level, slots, sems):
    core = position(where[0])[3]
    width = hidden.shape[1] // SIDE
    left = hidden.shape[0] - tokens
    copies = [
        pltpu.make_async_copy(
            hidden.at[pl.ds(0, tokens), pl.ds(b * width, width)], slots.at[b], sems.at[b]
        )
        for b in range(SIDE)
    ]
    later = [
        pltpu.make_async_copy(
            hidden.at[pl.ds(tokens, left), pl.ds(b * width, width)], rest.at[b], sems.at[SIDE + b]
        )
        for b in range(SIDE)
    ]
    for copy in copies + later:
        copy.start()
    top = None
    for b, copy in enumerate(copies):
        copy.wait()
        block = slots[b]
        top = highest(block, top)
        turned_rows(block, b, core, send, keep)
    level[...] = jnp.full((TAIL, 128), jnp.max(top.astype(jnp.float32)), jnp.float32)
    for copy in later:
        copy.wait()


def turn_first(tokens, where, hidden):
    count, width = hidden.shape
    out = pltpu.VMEM((SIDE, width // 8, tokens), hidden.dtype)
    return pl.pallas_call(
        functools.partial(turn_first_body, tokens),
        in_specs=[pl.BlockSpec(memory_space=pltpu.SMEM), pl.BlockSpec(memory_space=pltpu.HBM)],
        out_specs=[pl.BlockSpec(memory_space=pltpu.VMEM)] * 4,
        out_shape=[
            out,
            out,
            pltpu.VMEM((SIDE, count - tokens, width // SIDE), hidden.dtype),
            pltpu.VMEM((TAIL, 128), jnp.float32),
        ],
        scratch_shapes=[
            pltpu.VMEM((SIDE, tokens, width // SIDE), hidden.dtype),
            pltpu.SemaphoreType.DMA((2 * SIDE,)),
        ],
        compiler_params=pltpu.CompilerParams(vmem_limit_bytes=16 * 2**20),
        cost_estimate=pl.CostEstimate(flops=10**9, bytes_accessed=4 * 10**6, transcendentals=0),
    )(where, pltpu.with_memory_space_constraint(hidden, pltpu.HBM))


def turn_rest_body(where, rest, before, send, keep, level):
    core = position(where[0])[3]
    top = None
    for b in range(SIDE):
        block = rest[b]
        top = highest(block, top)
        turned_rows(block, b, core, send, keep)
    most = jnp.maximum(before[...], jnp.max(top.astype(jnp.float32)))
    level[...] = most
    units = 144 * SIDE
    for c in range(SIDE):
        send[c, units:] = most.astype(send.dtype)


def turn_rest(where, rest, before):
    tokens, width = rest.shape[1], rest.shape[2]
    return pl.pallas_call(
        turn_rest_body,
        in_specs=[pl.BlockSpec(memory_space=pltpu.SMEM)] + [pl.BlockSpec(memory_space=pltpu.VMEM)] * 2,
        out_specs=[pl.BlockSpec(memory_space=pltpu.VMEM)] * 3,
        out_shape=[
            pltpu.VMEM((SIDE, width // 2 + TAIL, tokens), rest.dtype),
            pltpu.VMEM((SIDE, width // 2, tokens), rest.dtype),
            pltpu.VMEM((TAIL, 128), jnp.float32),
        ],
        compiler_params=pltpu.CompilerParams(vmem_limit_bytes=12 * 2**20),
        cost_estimate=pl.CostEstimate(flops=10**9, bytes_accessed=4 * 10**6, transcendentals=0),
    )(where, *map(near, (rest, before)))


def largest(values):
    return jnp.max(jnp.max(jnp.abs(values), axis=0, keepdims=True).astype(jnp.float32))


def rows_of(part, step, where, sources):
    z, x, y, core = position(where[0])
    if part == "wide":
        at = jnp.where(core == 0, x, y) + step & 3
        pieces = [source[at, 0:576] for source in sources]
    else:
        row = pl.multiple_of((z + step & 3) * 144, 16)
        pieces = [
            jnp.concatenate([source[t, pl.ds(row, 144)] for t in range(SIDE)], 0)
            for source in sources
        ]
    return jnp.concatenate(pieces, 1)


def product_body(jobs, units, grads, started, levels, where, *refs):
    refs = list(refs)
    sources = [refs.pop(0) for _ in range(units)]
    weights = [refs.pop(0) for _ in range(grads)]
    sums = [refs.pop(0) if started else None for _ in jobs]
    given = [refs.pop(0)] if levels != "bounds" else [refs.pop(0), refs.pop(0)]
    outs = [refs.pop(0) for _ in jobs]
    bits = None
    if levels == "bounds":
        top, other = given
        tokens = weights[0].shape[0]
        refs[0][0:TAIL] = top[...] * (largest(weights[0][...]) * tokens)
        refs[0][TAIL:] = jnp.full((TAIL, 128), largest(other[...]) * tokens, jnp.float32)
    elif levels == "make":
        got_top = sources[1][0, 576:].astype(jnp.float32)
        bound = given[0][0:TAIL] + given[0][TAIL:] * got_top
        bits = 15.0 - jnp.ceil(jnp.log2(jnp.maximum(bound, 2.0**-60)))
        refs[0][...] = bits
    else:
        bits = given[0][...]
    whole = weights[0][...] if grads == 1 else jnp.concatenate([w[...] for w in weights], 0)
    for (part, step), before, out in zip(jobs, sums, outs):
        left = rows_of(part, step, where, sources)
        columns = whole[:, :WIDE] if part == "wide" else whole[:, WIDE:]
        value = jnp.dot(left, columns, preferred_element_type=jnp.float32)
        if before is not None:
            value = before[...] + value
        if levels == "bounds" or step == 0:
            out[0:576] = value
        else:
            out[0:576] = value * jnp.exp2(bits)[0:1, 0:1]
            out[576:] = jnp.broadcast_to(bits[:, 0:1], (TAIL, out.shape[1]))


def product(jobs, where, sources, weights, levels, given, sums=()):
    tail = 0 if levels == "bounds" else TAIL
    outs = [
        pltpu.VMEM((576 + (tail if step else 0), WIDE if part == "wide" else NARROW), jnp.float32)
        for part, step in jobs
    ]
    if levels == "bounds":
        outs.append(pltpu.VMEM((2 * TAIL, 128), jnp.float32))
    elif levels == "make":
        outs.append(pltpu.VMEM((TAIL, 128), jnp.float32))
    inputs = [*sources, *weights, *sums, *given]
    tokens = sum(source.shape[2] for source in sources)
    flops = sum(2 * 576 * tokens * (WIDE if part == "wide" else NARROW) for part, _ in jobs)
    return pl.pallas_call(
        functools.partial(product_body, jobs, len(sources), len(weights), bool(sums), levels),
        in_specs=[pl.BlockSpec(memory_space=pltpu.SMEM)]
        + [pl.BlockSpec(memory_space=pltpu.VMEM)] * len(inputs),
        out_specs=[pl.BlockSpec(memory_space=pltpu.VMEM)] * len(outs),
        out_shape=outs,
        compiler_params=pltpu.CompilerParams(vmem_limit_bytes=12 * 2**20),
        cost_estimate=pl.CostEstimate(flops=flops, bytes_accessed=10**6, transcendentals=0),
    )(where, *map(near, inputs))


def power(part, rows):
    return jnp.exp2(-part[rows : rows + 1].astype(jnp.float32))


def total(own, parts, rows):
    value = own[0:rows]
    for part in parts:
        value = value + part[0:rows].astype(jnp.float32) * power(part, rows)
    return value


def spread_body(part, high, blocks, where, value, tails, before, *refs):
    z, x, y, core = position(where[0])
    swap = core == (0 if part == "wide" else 1)
    if blocks == 16:
        at = jnp.where(swap, z, x) if part == "wide" else y
        major, minor = jnp.where(swap, 4, 1), jnp.where(swap, 1, 4)
    else:
        at = jnp.where(swap, y, z) if part == "wide" else x
        major, minor = 1, 0
    outs, level, scratch = refs[0:4], refs[4], refs[5]
    width = value.shape[1]
    bits = jnp.minimum(jnp.min(tails[...], axis=0, keepdims=True), before[0:1]) - 2.0
    level[...] = jnp.broadcast_to(bits, (TAIL, 128))
    scale = jnp.exp2(bits)[0:1, 0:1]
    for i in range(blocks):
        scratch[i, 0:BLOCK] = value[BLOCK * i : BLOCK * (i + 1)]
    for k in range(SIDE):
        chunk = at + k & 3
        for t in range(blocks // SIDE):
            piece = scratch[chunk * major + t * minor, 0:BLOCK]
            outs[k][BLOCK * t : BLOCK * (t + 1)] = piece * scale if k else piece
        end = BLOCK * blocks // SIDE
        if high > end:
            outs[k][end:high] = jnp.zeros((high - end, width), jnp.float32)
        if k:
            outs[k][high:] = jnp.broadcast_to(bits[:, 0:1], (TAIL, width))


def spread(where, part, blocks, own, parts, own_bits):
    rows = BLOCK * blocks
    kept = -(-rows // SIDE // TAIL) * TAIL
    width = own.shape[1]
    tails = [piece[rows:, 0:128].astype(jnp.float32) for piece in parts]
    inputs = [total(own, parts, rows), jnp.concatenate(tails, 0), own_bits]
    out = pl.pallas_call(
        functools.partial(spread_body, part, kept, blocks),
        in_specs=[pl.BlockSpec(memory_space=pltpu.SMEM)] + [pl.BlockSpec(memory_space=pltpu.VMEM)] * 3,
        out_specs=[pl.BlockSpec(memory_space=pltpu.VMEM)] * 5,
        out_shape=[pltpu.VMEM((kept, width), jnp.float32)]
        + [pltpu.VMEM((kept + TAIL, width), jnp.float32)] * 3
        + [pltpu.VMEM((TAIL, 128), jnp.float32)],
        scratch_shapes=[pltpu.VMEM((blocks, PADDED, width), jnp.float32)],
        compiler_params=pltpu.CompilerParams(vmem_limit_bytes=12 * 2**20),
        cost_estimate=pl.CostEstimate(flops=10**8, bytes_accessed=10**7, transcendentals=0),
    )(where, *map(near, inputs))
    return out[:4], out[4]


def exchange(chunks, dims):
    arrived = {}
    for k in chunks:
        arrived[k] = lax.ppermute(chunks[k].astype(jnp.float16), AXES, routes(dims, k))
    return arrived


def input_gradient_body(grad, weight, out, loads, stores, load_sems, store_sems):
    count, step = loads.shape[0], loads.shape[1]
    incoming = [
        pltpu.make_async_copy(weight.at[pl.ds(i * step, step)], loads.at[i], load_sems.at[i])
        for i in range(count)
    ]
    outgoing = [
        pltpu.make_async_copy(stores.at[i], out.at[:, pl.ds(i * step, step)], store_sems.at[i])
        for i in range(count)
    ]
    for copy in incoming:
        copy.start()
    for i in range(count):
        incoming[i].wait()
        stores[i] = lax.dot_general(
            grad[...], loads[i], (((1,), (1,)), ((), ())), preferred_element_type=jnp.float32
        ).astype(out.dtype)
        outgoing[i].start()
    for copy in outgoing:
        copy.wait()


def input_gradient(grad, weight):
    tokens, width = grad.shape
    features = weight.shape[0]
    count = 9
    return pl.pallas_call(
        input_gradient_body,
        in_specs=[pl.BlockSpec(memory_space=pltpu.VMEM), pl.BlockSpec(memory_space=pltpu.HBM)],
        out_specs=pl.BlockSpec(memory_space=pltpu.HBM),
        out_shape=pltpu.HBM((tokens, features), grad.dtype),
        scratch_shapes=[
            pltpu.VMEM((count, features // count, width), weight.dtype),
            pltpu.VMEM((count, tokens, features // count), grad.dtype),
            pltpu.SemaphoreType.DMA((count,)),
            pltpu.SemaphoreType.DMA((count,)),
        ],
        compiler_params=pltpu.CompilerParams(vmem_limit_bytes=18 * 2**20),
        cost_estimate=pl.CostEstimate(
            flops=2 * tokens * width * features, bytes_accessed=15 * 10**6, transcendentals=0
        ),
    )(near(grad), pltpu.with_memory_space_constraint(weight, pltpu.HBM))


def listed(parts):
    return [parts[k] for k in (1, 2, 3)]


def body(hidden, out_grad, down_weight):
    where = lax.axis_index(AXES).reshape(1)
    tokens = hidden.shape[0] * 128
    factor = 1.0 / float(tokens) ** 0.5

    other_grad = across_cores(out_grad)
    send_one, keep_one, rest, top = turn_first(256, where, hidden)
    got_one = across_cores(send_one)
    send_two, keep_two, top = turn_rest(where, rest, top)
    got_two = across_cores(send_two)
    kept, got = (keep_one, keep_two), (got_one, got_two)

    early = (("wide", 1), ("wide", 3), ("narrow", 1), ("narrow", 3))
    *sums, bounds = product(early, where, kept, [out_grad], "bounds", [top, other_grad])
    arrived = {"wide": {}, "narrow": {}}
    level = None
    for jobs, started in ((early[:1], sums[:1]), (early[1:2], sums[1:2]), (early[2:], sums[2:])):
        if level is None:
            value, level = product(jobs, where, got, [other_grad], "make", [bounds], started)
            values = [value]
        else:
            values = product(jobs, where, got, [other_grad], "use", [level], started)
        for (part, k), value in zip(jobs, values):
            arrived[part] |= exchange({k: value}, FIRST[part])
    both, grads = (*kept, *got), [out_grad, other_grad]
    jobs = (("wide", 2), ("narrow", 2))
    values = product(jobs, where, both, grads, "use", [level])
    for (part, k), value in zip(jobs, values):
        arrived[part] |= exchange({k: value}, FIRST[part])

    hidden_grad = input_gradient(out_grad, down_weight)
    stay = product((("wide", 0), ("narrow", 0)), where, both, grads, "use", [level])

    columns = []
    for part, own in zip(PARTS, stay):
        (own, *chunks), bits = spread(where, part, 16, own, listed(arrived[part]), level)
        parts = exchange({k: chunks[k - 1] for k in LATE}, SECOND[part])
        (own, *chunks), bits = spread(where, part, 4, own, listed(parts), bits)
        parts = exchange({k: chunks[k - 1] for k in LATE}, THIRD[part])
        columns.append(total(own, listed(parts), PADDED)[0:BLOCK])
    weight_grad = jnp.concatenate(columns, 1) * factor
    return (weight_grad, hidden_grad)


def solution(mesh):
    in_specs = (P(AXES, None), P(AXES, None), P())
    out_specs = (P(AXES, None), P(AXES, None))
    return jax.shard_map(body, mesh=mesh, in_specs=in_specs, out_specs=out_specs, check_vma=False)
```

```python
import functools

import jax
import jax.numpy as jnp
from jax import lax
from jax.experimental import pallas as pl
from jax.experimental.pallas import tpu as pltpu
from jax.sharding import PartitionSpec as P


AXES = ("gx", "gy", "gz")
SIDE = 4
BLOCK = 36
PADDED = 40
TAIL = 8
LATE = (2, 1, 3)
FIRST = {"wide": "xy", "narrow": "zz"}
SECOND = {"wide": "zx", "narrow": "yy"}
THIRD = {"wide": "yz", "narrow": "xx"}
PARTS = ("narrow", "wide")
WIDE = 768
NARROW = 384


def near(array):
    return pltpu.with_memory_space_constraint(array, pltpu.VMEM)


def position(index):
    return index >> 5, index >> 3 & 3, index >> 1 & 2 | index & 1, index >> 1 & 1


def device(z, x, y, core):
    return ((z * 4 + x) * 4 + y // 2 * 2 + core) * 2 + y % 2


def routes(dims, step):
    pairs = []
    for source in range(128):
        at = dict(zip("zxyc", position(source)))
        along = dims[at["c"]]
        at[along] = (at[along] + step) % SIDE
        pairs.append((source, device(at["z"], at["x"], at["y"], at["c"])))
    return pairs


def across_cores(array):
    pairs = []
    for source in range(128):
        z, x, y, core = position(source)
        pairs.append((source, device(z, x, y, 1 - core)))
    return lax.ppermute(array, AXES, pairs)


def turned_rows(block, b, core, send, keep):
    turned = block.T
    for x in range(SIDE):
        rows = 288 * x
        piece = jnp.concatenate([turned[rows : rows + 72], turned[rows + 144 : rows + 216]], 0)

        @pl.when(core == 0)
        def _():
            keep[x, 144 * b : 144 * (b + 1)] = piece

        @pl.when(core == 1)
        def _():
            send[x, 144 * b : 144 * (b + 1)] = piece

    for y in range(SIDE):
        rows = 144 * (y // 2) + 72 + BLOCK * (y % 2)
        piece = jnp.concatenate(
            [turned[288 * x + rows : 288 * x + rows + BLOCK] for x in range(SIDE)], 0
        )

        @pl.when(core == 1)
        def _():
            keep[y, 144 * b : 144 * (b + 1)] = piece

        @pl.when(core == 0)
        def _():
            send[y, 144 * b : 144 * (b + 1)] = piece


def highest(block, top):
    most = jnp.max(jnp.abs(block), axis=0, keepdims=True)
    return most if top is None else jnp.maximum(top, most)


def turn_first_body(tokens, where, hidden, send, keep, rest, level, slots, sems):
    core = position(where[0])[3]
    width = hidden.shape[1] // SIDE
    left = hidden.shape[0] - tokens
    copies = [
        pltpu.make_async_copy(
            hidden.at[pl.ds(0, tokens), pl.ds(b * width, width)], slots.at[b], sems.at[b]
        )
        for b in range(SIDE)
    ]
    later = [
        pltpu.make_async_copy(
            hidden.at[pl.ds(tokens, left), pl.ds(b * width, width)], rest.at[b], sems.at[SIDE + b]
        )
        for b in range(SIDE)
    ]
    for copy in copies + later:
        copy.start()
    top = None
    for b, copy in enumerate(copies):
        copy.wait()
        block = slots[b]
        top = highest(block, top)
        turned_rows(block, b, core, send, keep)
    level[...] = jnp.full((TAIL, 128), jnp.max(top.astype(jnp.float32)), jnp.float32)
    for copy in later:
        copy.wait()


def turn_first(tokens, where, hidden):
    count, width = hidden.shape
    out = pltpu.VMEM((SIDE, width // 8, tokens), hidden.dtype)
    return pl.pallas_call(
        functools.partial(turn_first_body, tokens),
        in_specs=[pl.BlockSpec(memory_space=pltpu.SMEM), pl.BlockSpec(memory_space=pltpu.HBM)],
        out_specs=[pl.BlockSpec(memory_space=pltpu.VMEM)] * 4,
        out_shape=[
            out,
            out,
            pltpu.VMEM((SIDE, count - tokens, width // SIDE), hidden.dtype),
            pltpu.VMEM((TAIL, 128), jnp.float32),
        ],
        scratch_shapes=[
            pltpu.VMEM((SIDE, tokens, width // SIDE), hidden.dtype),
            pltpu.SemaphoreType.DMA((2 * SIDE,)),
        ],
        compiler_params=pltpu.CompilerParams(vmem_limit_bytes=16 * 2**20),
        cost_estimate=pl.CostEstimate(flops=10**9, bytes_accessed=4 * 10**6, transcendentals=0),
    )(where, pltpu.with_memory_space_constraint(hidden, pltpu.HBM))


def turn_rest_body(where, rest, before, send, keep, level):
    core = position(where[0])[3]
    top = None
    for b in range(SIDE):
        block = rest[b]
        top = highest(block, top)
        turned_rows(block, b, core, send, keep)
    most = jnp.maximum(before[...], jnp.max(top.astype(jnp.float32)))
    level[...] = most
    units = 144 * SIDE
    for c in range(SIDE):
        send[c, units:] = most.astype(send.dtype)


def turn_rest(where, rest, before):
    tokens, width = rest.shape[1], rest.shape[2]
    return pl.pallas_call(
        turn_rest_body,
        in_specs=[pl.BlockSpec(memory_space=pltpu.SMEM)] + [pl.BlockSpec(memory_space=pltpu.VMEM)] * 2,
        out_specs=[pl.BlockSpec(memory_space=pltpu.VMEM)] * 3,
        out_shape=[
            pltpu.VMEM((SIDE, width // 2 + TAIL, tokens), rest.dtype),
            pltpu.VMEM((SIDE, width // 2, tokens), rest.dtype),
            pltpu.VMEM((TAIL, 128), jnp.float32),
        ],
        compiler_params=pltpu.CompilerParams(vmem_limit_bytes=12 * 2**20),
        cost_estimate=pl.CostEstimate(flops=10**9, bytes_accessed=4 * 10**6, transcendentals=0),
    )(where, *map(near, (rest, before)))


def largest(values):
    return jnp.max(jnp.max(jnp.abs(values), axis=0, keepdims=True).astype(jnp.float32))


def rows_of(part, step, where, sources):
    z, x, y, core = position(where[0])
    if part == "wide":
        at = jnp.where(core == 0, x, y) + step & 3
        pieces = [source[at, 0:576] for source in sources]
    else:
        row = pl.multiple_of((z + step & 3) * 144, 16)
        pieces = [
            jnp.concatenate([source[t, pl.ds(row, 144)] for t in range(SIDE)], 0)
            for source in sources
        ]
    return jnp.concatenate(pieces, 1)


def product_body(jobs, units, grads, started, levels, where, *refs):
    refs = list(refs)
    sources = [refs.pop(0) for _ in range(units)]
    weights = [refs.pop(0) for _ in range(grads)]
    sums = [refs.pop(0) if started else None for _ in jobs]
    given = [refs.pop(0)] if levels != "bounds" else [refs.pop(0), refs.pop(0)]
    outs = [refs.pop(0) for _ in jobs]
    bits = None
    if levels == "bounds":
        top, other = given
        tokens = weights[0].shape[0]
        refs[0][0:TAIL] = top[...] * (largest(weights[0][...]) * tokens)
        refs[0][TAIL:] = jnp.full((TAIL, 128), largest(other[...]) * tokens, jnp.float32)
    elif levels == "make":
        got_top = sources[1][0, 576:].astype(jnp.float32)
        bound = given[0][0:TAIL] + given[0][TAIL:] * got_top
        bits = 15.0 - jnp.ceil(jnp.log2(jnp.maximum(bound, 2.0**-60)))
        refs[0][...] = bits
    else:
        bits = given[0][...]
    whole = weights[0][...] if grads == 1 else jnp.concatenate([w[...] for w in weights], 0)
    for (part, step), before, out in zip(jobs, sums, outs):
        left = rows_of(part, step, where, sources)
        columns = whole[:, :WIDE] if part == "wide" else whole[:, WIDE:]
        value = jnp.dot(left, columns, preferred_element_type=jnp.float32)
        if before is not None:
            value = before[...] + value
        if levels == "bounds" or step == 0:
            out[0:576] = value
        else:
            out[0:576] = value * jnp.exp2(bits)[0:1, 0:1]
            out[576:] = jnp.broadcast_to(bits[:, 0:1], (TAIL, out.shape[1]))


def product(jobs, where, sources, weights, levels, given, sums=()):
    tail = 0 if levels == "bounds" else TAIL
    outs = [
        pltpu.VMEM((576 + (tail if step else 0), WIDE if part == "wide" else NARROW), jnp.float32)
        for part, step in jobs
    ]
    if levels == "bounds":
        outs.append(pltpu.VMEM((2 * TAIL, 128), jnp.float32))
    elif levels == "make":
        outs.append(pltpu.VMEM((TAIL, 128), jnp.float32))
    inputs = [*sources, *weights, *sums, *given]
    tokens = sum(source.shape[2] for source in sources)
    flops = sum(2 * 576 * tokens * (WIDE if part == "wide" else NARROW) for part, _ in jobs)
    return pl.pallas_call(
        functools.partial(product_body, jobs, len(sources), len(weights), bool(sums), levels),
        in_specs=[pl.BlockSpec(memory_space=pltpu.SMEM)]
        + [pl.BlockSpec(memory_space=pltpu.VMEM)] * len(inputs),
        out_specs=[pl.BlockSpec(memory_space=pltpu.VMEM)] * len(outs),
        out_shape=outs,
        compiler_params=pltpu.CompilerParams(vmem_limit_bytes=12 * 2**20),
        cost_estimate=pl.CostEstimate(flops=flops, bytes_accessed=10**6, transcendentals=0),
    )(where, *map(near, inputs))


def power(part, rows):
    return jnp.exp2(-part[rows : rows + 1].astype(jnp.float32))


def total(own, parts, rows):
    value = own[0:rows]
    for part in parts:
        value = value + part[0:rows].astype(jnp.float32) * power(part, rows)
    return value


def spread_body(part, high, blocks, where, value, tails, before, *refs):
    z, x, y, core = position(where[0])
    swap = core == (0 if part == "wide" else 1)
    if blocks == 16:
        at = jnp.where(swap, z, x) if part == "wide" else y
        major, minor = jnp.where(swap, 4, 1), jnp.where(swap, 1, 4)
    else:
        at = jnp.where(swap, y, z) if part == "wide" else x
        major, minor = 1, 0
    outs, level, scratch = refs[0:4], refs[4:-1], refs[-1]
    width = value.shape[1]
    bits = jnp.minimum(jnp.min(tails[...], axis=0, keepdims=True), before[0:1]) - 2.0
    if level:
        level[0][...] = jnp.broadcast_to(bits, (TAIL, 128))
    scale = jnp.exp2(bits)[0:1, 0:1]
    for i in range(blocks):
        scratch[i, 0:BLOCK] = value[BLOCK * i : BLOCK * (i + 1)]
    for k in range(SIDE):
        chunk = at + k & 3
        for t in range(blocks // SIDE):
            piece = scratch[chunk * major + t * minor, 0:BLOCK]
            outs[k][BLOCK * t : BLOCK * (t + 1)] = piece * scale if k else piece
        end = BLOCK * blocks // SIDE
        if high > end:
            outs[k][end:high] = jnp.zeros((high - end, width), jnp.float32)
        if k:
            outs[k][high:] = jnp.broadcast_to(bits[:, 0:1], (TAIL, width))


def spread(where, part, blocks, own, parts, own_bits):
    rows = BLOCK * blocks
    kept = -(-rows // SIDE // TAIL) * TAIL
    width = own.shape[1]
    tails = [piece[rows:, 0:128].astype(jnp.float32) for piece in parts]
    inputs = [total(own, parts, rows), jnp.concatenate(tails, 0), own_bits]
    out = pl.pallas_call(
        functools.partial(spread_body, part, kept, blocks),
        in_specs=[pl.BlockSpec(memory_space=pltpu.SMEM)] + [pl.BlockSpec(memory_space=pltpu.VMEM)] * 3,
        out_specs=[pl.BlockSpec(memory_space=pltpu.VMEM)] * (5 if blocks > SIDE else 4),
        out_shape=[pltpu.VMEM((kept, width), jnp.float32)]
        + [pltpu.VMEM((kept + TAIL, width), jnp.float32)] * 3
        + [pltpu.VMEM((TAIL, 128), jnp.float32)] * (blocks > SIDE),
        scratch_shapes=[pltpu.VMEM((blocks, PADDED, width), jnp.float32)],
        compiler_params=pltpu.CompilerParams(vmem_limit_bytes=12 * 2**20),
        cost_estimate=pl.CostEstimate(flops=10**8, bytes_accessed=10**7, transcendentals=0),
    )(where, *map(near, inputs))
    return out[:4], out[4:]


def exchange(chunks, dims):
    arrived = {}
    for k in chunks:
        arrived[k] = lax.ppermute(chunks[k].astype(jnp.float16), AXES, routes(dims, k))
    return arrived


def input_gradient_body(grad, weight, out, loads, stores, load_sems, store_sems):
    count, step = loads.shape[0], loads.shape[1]
    incoming = [
        pltpu.make_async_copy(weight.at[pl.ds(i * step, step)], loads.at[i], load_sems.at[i])
        for i in range(count)
    ]
    outgoing = [
        pltpu.make_async_copy(stores.at[i], out.at[:, pl.ds(i * step, step)], store_sems.at[i])
        for i in range(count)
    ]
    for copy in incoming:
        copy.start()
    for i in range(count):
        incoming[i].wait()
        stores[i] = lax.dot_general(
            grad[...], loads[i], (((1,), (1,)), ((), ())), preferred_element_type=jnp.float32
        ).astype(out.dtype)
        outgoing[i].start()
    for copy in outgoing:
        copy.wait()


def input_gradient(grad, weight):
    tokens, width = grad.shape
    features = weight.shape[0]
    count = 9
    return pl.pallas_call(
        input_gradient_body,
        in_specs=[pl.BlockSpec(memory_space=pltpu.VMEM), pl.BlockSpec(memory_space=pltpu.HBM)],
        out_specs=pl.BlockSpec(memory_space=pltpu.HBM),
        out_shape=pltpu.HBM((tokens, features), grad.dtype),
        scratch_shapes=[
            pltpu.VMEM((count, features // count, width), weight.dtype),
            pltpu.VMEM((count, tokens, features // count), grad.dtype),
            pltpu.SemaphoreType.DMA((count,)),
            pltpu.SemaphoreType.DMA((count,)),
        ],
        compiler_params=pltpu.CompilerParams(vmem_limit_bytes=18 * 2**20),
        cost_estimate=pl.CostEstimate(
            flops=2 * tokens * width * features, bytes_accessed=15 * 10**6, transcendentals=0
        ),
    )(near(grad), pltpu.with_memory_space_constraint(weight, pltpu.HBM))


def listed(parts):
    return [parts[k] for k in (1, 2, 3)]


def body(hidden, out_grad, down_weight):
    where = lax.axis_index(AXES).reshape(1)
    tokens = hidden.shape[0] * 128
    factor = 1.0 / float(tokens) ** 0.5

    other_grad = across_cores(out_grad)
    send_one, keep_one, rest, top = turn_first(256, where, hidden)
    got_one = across_cores(send_one)
    send_two, keep_two, top = turn_rest(where, rest, top)
    got_two = across_cores(send_two)
    kept, got = (keep_one, keep_two), (got_one, got_two)

    early = (("narrow", 1), ("narrow", 3), ("wide", 1), ("wide", 3))
    *sums, bounds = product(early, where, kept, [out_grad], "bounds", [top, other_grad])
    arrived = {part: {} for part in PARTS}
    level = None
    for jobs, started in ((early[:2], sums[:2]), (early[2:3], sums[2:3]), (early[3:], sums[3:])):
        if level is None:
            *values, level = product(jobs, where, got, [other_grad], "make", [bounds], started)
        else:
            values = product(jobs, where, got, [other_grad], "use", [level], started)
        for (part, k), value in zip(jobs, values):
            arrived[part] |= exchange({k: value}, FIRST[part])
    both, grads = (*kept, *got), [out_grad, other_grad]
    jobs = tuple((part, 2) for part in PARTS)
    values = product(jobs, where, both, grads, "use", [level])
    for (part, k), value in zip(jobs, values):
        arrived[part] |= exchange({k: value}, FIRST[part])

    hidden_grad = input_gradient(out_grad, down_weight)
    stay = product(tuple((part, 0) for part in PARTS), where, both, grads, "use", [level])

    columns = {}
    for part, own in zip(PARTS, stay):
        (own, *chunks), (bits,) = spread(where, part, 16, own, listed(arrived[part]), level)
        parts = exchange({k: chunks[k - 1] for k in LATE}, SECOND[part])
        (own, *chunks), _ = spread(where, part, 4, own, listed(parts), bits)
        parts = exchange({k: chunks[k - 1] for k in LATE}, THIRD[part])
        columns[part] = total(own, listed(parts), PADDED)[0:BLOCK]
    weight_grad = jnp.concatenate([columns["wide"], columns["narrow"]], 1) * factor
    return (weight_grad, hidden_grad)


def solution(mesh):
    in_specs = (P(AXES, None), P(AXES, None), P())
    out_specs = (P(AXES, None), P(AXES, None))
    return jax.shard_map(body, mesh=mesh, in_specs=in_specs, out_specs=out_specs, check_vma=False)
```
